32 devices in a mesh: img: 32 (over z, y, x, core).
Axes of the slice: x: 2, y: 2, z: 4, core: 2. Of those that a mesh axis runs over, the one named last changes fastest.
Arguments:
- queries: bfloat16 [12288, 1024], P('img'), may hold values from -10 to 10
- keys: bfloat16 [12288, 1024], P('img'), may hold values from -10 to 10
- values: bfloat16 [12288, 1024], P('img'), may hold values from -6 to 6
- out_grad: bfloat16 [12288, 1024], P('img'), may hold values from -6 to 6
- image_ids: int32 [12288], P('img'), may hold values from 0 to 31, never falling along the last dimension, each value on 1 to 1152 neighbouring positions
Outputs:
- attended: bfloat16 [12288, 1024], P('img')
- query_grad: bfloat16 [12288, 1024], P('img')
- key_grad: bfloat16 [12288, 1024], P('img')
- value_grad: bfloat16 [12288, 1024], P('img')
The draws below stay inside these ranges and needn't reach their ends.
Inputs may be any that keep to these rules, and one draw needn't show every extreme that they name: `image_ids`: the regions of one image stand in consecutive rows, and ids rise along the rows; an image has 1 to 1152 regions, and some image has exactly 1152.
All inputs are finite; a program needn't handle non-finite values.
Results may differ from the reference program's by a relative error of at most 0.0069.
Values may be sent and summed in bfloat16 or wider, within the bound.
A program may use at most 192 MiB of HBM per device.

```python
import math
import jax
import jax.numpy as jnp
import numpy as np
from jax import lax

D = 1024
HEADS = 16
ROWS_DEV = 384
REACH = 3
MOST = 1152
TOKENS = 12288
N_IMG = 32


def paired_features(key):
    base = jax.random.fold_in(key, 7)
    first, second = jax.random.split(base, 2)
    shape = (TOKENS, D)
    query_f = jnp.clip(jax.random.normal(first, shape, jnp.float32), -6.0, 6.0)
    key_f = jnp.clip(jax.random.normal(second, shape, jnp.float32), -6.0, 6.0)
    return (query_f, key_f)


def draw_queries(key, part):
    return paired_features(key)[0].astype(jnp.bfloat16)


def draw_keys(key, part):
    return paired_features(key)[1].astype(jnp.bfloat16)


def levels(key, extent, cuts, least, top_value):
    gain = 1.0
    for axis_at, shards_of in cuts:
        steps = jax.random.uniform(jax.random.fold_in(jax.random.fold_in(key, 6), axis_at), (shards_of,), jnp.float32, least / len(cuts), top_value / len(cuts))
        gain = gain * jnp.repeat(jnp.exp(steps), extent[axis_at] // shards_of).reshape((-1,) + (1,) * (len(extent) - 1 - axis_at))
    return gain


def profile(amount, total, limit, lean):
    portions = [(1 << 20) // math.isqrt(rank ** lean) + 1 for rank in range(2, amount + 1)]
    spare, holding = total - limit - (amount - 1), [1] * (amount - 1)
    while spare > 0:
        free = [i for i in range(amount - 1) if holding[i] < limit]
        pool, remaining = sum([portions[i] for i in free]), spare
        for i in free:
            more = min(limit - holding[i], max(1, remaining * portions[i] // pool), spare)
            holding[i] = holding[i] + more
            spare = spare - more
    return np.array([limit] + holding)


def ragged_sizes(own_key, amount, total, limit, lean):
    if amount == 2:
        one = jax.random.randint(own_key, (), max(1, total - limit), min(limit, total - 1) + 1)
        return jnp.stack([one, total - one])
    tallies = jnp.asarray(profile(amount, total, limit, lean), jnp.int32)
    twos = (amount - 1) // 2
    donor, taker = tallies[1:1 + 2 * twos:2], tallies[2:2 + 2 * twos:2]
    room = jnp.minimum(donor - 1, limit - taker)
    shifted = jax.random.randint(jax.random.fold_in(own_key, 1), (twos,), 0, 1 << 20) % (room + 1)
    tallies = tallies.at[1:1 + 2 * twos:2].set(donor - shifted).at[2:2 + 2 * twos:2].set(taker + shifted)
    return tallies[jax.random.permutation(jax.random.fold_in(own_key, 2), amount)]


def bell_draw(own_key, dims, spread, reach, cuts=(), held_as=jnp.bfloat16):
    drawn = spread * jax.random.normal(own_key, dims, jnp.float32)
    if cuts:
        drawn = drawn * levels(own_key, dims, cuts, -0.22, 0.18)
    return jnp.clip(drawn, -reach, reach).astype(held_as)


def setup_inputs(seed: int = 0) -> dict:
    arg_keys = jax.random.split(jax.random.key(seed), 6)
    return {
        "queries": draw_queries(jax.random.fold_in(arg_keys[5], 71), 0),
        "keys": draw_keys(jax.random.fold_in(arg_keys[5], 71), 0),
        "values": bell_draw(arg_keys[2], (TOKENS, D), 1.0, 6.0, ((0, 32),)),
        "out_grad": bell_draw(arg_keys[3], (TOKENS, D), 1.0, 6.0, ((0, 32),)),
        "image_ids": jnp.searchsorted(jnp.cumsum(ragged_sizes(arg_keys[4], N_IMG, TOKENS, MOST, 1)), jnp.arange(TOKENS), side="right").astype(jnp.int32),
    }


def attend_block(query_rows, key_rows, value_rows, grad_rows, query_tags, key_tags):
    row_count = query_rows.shape[0]
    width = key_rows.shape[0]
    head_dim = D // HEADS
    score_scale = 1.0 / math.sqrt(head_dim)
    query_f = query_rows.astype(jnp.float32).reshape(row_count, HEADS, head_dim)
    key_f = key_rows.astype(jnp.float32).reshape(width, HEADS, head_dim)
    value_f = value_rows.astype(jnp.float32).reshape(width, HEADS, head_dim)
    grad_f = grad_rows.astype(jnp.float32).reshape(row_count, HEADS, head_dim)
    same_image = query_tags[:, None] == key_tags[None, :]
    scores = jnp.einsum('rhd,whd->hrw', query_f, key_f) * score_scale
    scores = jnp.where(same_image[None], scores, -1e+30)
    peak = lax.optimization_barrier(jnp.max(scores, axis=-1, keepdims=True))
    weights = jnp.exp(scores - peak)
    probs = weights / lax.optimization_barrier(jnp.sum(weights, axis=-1, keepdims=True))
    probs_b = lax.optimization_barrier(probs.astype(jnp.bfloat16)).astype(jnp.float32)
    attended = jnp.einsum('hrw,whd->rhd', probs_b, value_f).reshape(row_count, D).astype(jnp.bfloat16)
    dprobs = jnp.einsum('rhd,whd->hrw', grad_f, value_f)
    row_delta = lax.optimization_barrier(jnp.sum(probs * dprobs, axis=-1, keepdims=True))
    dscores = probs * (dprobs - row_delta)
    dscores_b = lax.optimization_barrier(dscores.astype(jnp.bfloat16)).astype(jnp.float32)
    query_grad = (jnp.einsum('hrw,whd->rhd', dscores_b, key_f) * score_scale).reshape(row_count, D).astype(jnp.bfloat16)
    key_grad = (jnp.einsum('hrw,rhd->whd', dscores_b, query_f) * score_scale).reshape(width, D)
    value_grad = jnp.einsum('hrw,rhd->whd', probs_b, grad_f).reshape(width, D)
    return (attended, query_grad, key_grad, value_grad)

def reference(queries, keys, values, out_grad, image_ids):
    row_count = ROWS_DEV
    width = (2 * REACH + 1) * row_count
    margin = REACH * row_count
    image_tags = (image_ids + 1).astype(jnp.int32)
    keys_padded = jnp.pad(keys, ((margin, margin), (0, 0)))
    values_padded = jnp.pad(values, ((margin, margin), (0, 0)))
    tags_padded = jnp.pad(image_tags, (margin, margin))
    start_acc = (jnp.zeros((TOKENS + 2 * margin, D), jnp.float32), jnp.zeros((TOKENS + 2 * margin, D), jnp.float32))

    def one_block(carry, block):
        key_acc, value_acc = carry
        start = (block * row_count).astype(jnp.int32)
        query_rows = lax.dynamic_slice_in_dim(queries, start, row_count, 0)
        grad_rows = lax.dynamic_slice_in_dim(out_grad, start, row_count, 0)
        query_tags = lax.dynamic_slice_in_dim(image_tags, start, row_count, 0)
        key_rows = lax.dynamic_slice_in_dim(keys_padded, start, width, 0)
        value_rows = lax.dynamic_slice_in_dim(values_padded, start, width, 0)
        key_tags = lax.dynamic_slice_in_dim(tags_padded, start, width, 0)
        attended, query_grad, key_grad, value_grad = attend_block(query_rows, key_rows, value_rows, grad_rows, query_tags, key_tags)
        key_acc = lax.dynamic_update_slice_in_dim(key_acc, lax.dynamic_slice_in_dim(key_acc, start, width, 0) + key_grad, start, 0)
        value_acc = lax.dynamic_update_slice_in_dim(value_acc, lax.dynamic_slice_in_dim(value_acc, start, width, 0) + value_grad, start, 0)
        return ((key_acc, value_acc), (attended, query_grad))
    (key_acc, value_acc), (attended, query_grad) = lax.scan(one_block, start_acc, jnp.arange(N_IMG, dtype=jnp.int32))
    attended = attended.reshape(TOKENS, D)
    query_grad = query_grad.reshape(TOKENS, D)
    key_grad = key_acc[margin:margin + TOKENS].astype(jnp.bfloat16)
    value_grad = value_acc[margin:margin + TOKENS].astype(jnp.bfloat16)
    return (attended, query_grad, key_grad, value_grad)
```

```python
import math

import jax
import jax.numpy as jnp
from jax import lax
from jax.experimental import pallas as pl
from jax.experimental.pallas import tpu as pltpu
from jax.sharding import PartitionSpec as P

HEAD_DIM = 64
REACH = 3
LANES = 128
TQ = 128
TK = 256
NO_TAG = 1 << 30


def dot_nt(a, b):
    return lax.dot_general(a, b, (((1,), (1,)), ((), ())), preferred_element_type=jnp.float32)


def dot_nn(a, b):
    return lax.dot_general(a, b, (((1,), (0,)), ((), ())), preferred_element_type=jnp.float32)


def attend_kernel(
    tags_s, bounds, q_ref, k_ref, v_ref, g_ref, kt_ref, vt_ref, tag_cols, tag_rows,
    att_ref, dq_ref, dk_ref, dv_ref,
    s_buf, dp_buf, dk_acc, dv_acc, att_acc, dq_acc,
):
    dk_acc[...] = jnp.zeros_like(dk_acc)
    dv_acc[...] = jnp.zeros_like(dv_acc)
    low = lax.broadcasted_iota(jnp.int32, (TQ, LANES), 1) < HEAD_DIM
    scale = 1.0 / math.sqrt(HEAD_DIM)
    all_tags = tag_rows[...]

    def one_tile(tile, carry):
        row0 = pl.multiple_of(tile * TQ, TQ)
        rows = pl.ds(row0, TQ)
        first_tag = tags_s[row0]
        last_tag = tags_s[row0 + TQ - 1]
        key_begin = jnp.sum((all_tags < first_tag).astype(jnp.int32))
        key_end = jnp.sum((all_tags <= last_tag).astype(jnp.int32))
        key0 = (key_begin // LANES) * LANES
        steps = (key_end - key0 + TK - 1) // TK
        q = q_ref[rows, :].astype(jnp.float32) * scale
        g = g_ref[rows, :].astype(jnp.float32)
        q2 = jnp.concatenate(
            [jnp.where(low, q, 0.0), jnp.where(low, 0.0, q)], 0).astype(jnp.bfloat16)
        g2 = jnp.concatenate(
            [jnp.where(low, g, 0.0), jnp.where(low, 0.0, g)], 0).astype(jnp.bfloat16)
        q_tags = tag_rows[pl.ds(tile, 1), :]

        def score_step(j, peak):
            keys = pl.ds(pl.multiple_of(key0 + j * TK, LANES), TK)
            held = pl.ds(pl.multiple_of(j * TK, TK), TK)
            s = dot_nt(k_ref[keys, :], q2)
            same = tag_cols[keys, :] == q_tags
            s = jnp.concatenate(
                [jnp.where(same, s[:, :TQ], -1e30), jnp.where(same, s[:, TQ:], -1e30)], 1)
            s_buf[held, :] = s
            dp_buf[held, :] = dot_nt(v_ref[keys, :], g2)
            return jnp.maximum(peak, jnp.max(s.reshape(TK // 8, 8, 2 * TQ), 0))

        peak = lax.fori_loop(0, steps, score_step, jnp.full((8, 2 * TQ), -1e30, jnp.float32))
        peak = jnp.max(peak, 0, keepdims=True)

        def weight_step(j, sums):
            total, delta = sums
            held = pl.ds(pl.multiple_of(j * TK, TK), TK)
            w = jnp.exp(s_buf[held, :] - peak)
            s_buf[held, :] = w
            wd = w * dp_buf[held, :]
            total = total + jnp.sum(w.reshape(TK // 8, 8, 2 * TQ), 0)
            delta = delta + jnp.sum(wd.reshape(TK // 8, 8, 2 * TQ), 0)
            return total, delta

        zero = jnp.zeros((8, 2 * TQ), jnp.float32)
        total, delta = lax.fori_loop(0, steps, weight_step, (zero, zero))
        inverse = 1.0 / jnp.sum(total, 0, keepdims=True)
        delta = jnp.sum(delta, 0, keepdims=True) * inverse
        att_acc[...] = jnp.zeros_like(att_acc)
        dq_acc[...] = jnp.zeros_like(dq_acc)

        def grad_step(j, c):
            keys = pl.ds(pl.multiple_of(key0 + j * TK, LANES), TK)
            held = pl.ds(pl.multiple_of(j * TK, TK), TK)
            p = s_buf[held, :] * inverse
            ds = (p * (dp_buf[held, :] - delta)).astype(jnp.bfloat16)
            p = p.astype(jnp.bfloat16)
            att_acc[...] += dot_nn(vt_ref[:, keys], p)
            dq_acc[...] += dot_nn(kt_ref[:, keys], ds)
            dv_acc[keys, :] += dot_nn(p, g2)
            dk_acc[keys, :] += dot_nn(ds, q2)
            return c

        lax.fori_loop(0, steps, grad_step, 0)
        att = att_acc[...]
        dq = dq_acc[...] * scale
        top = lax.broadcasted_iota(jnp.int32, (LANES, TQ), 0) < HEAD_DIM
        att_ref[rows, :] = jnp.where(top, att[:, :TQ], att[:, TQ:]).T.astype(jnp.bfloat16)
        dq_ref[rows, :] = jnp.where(top, dq[:, :TQ], dq[:, TQ:]).T.astype(jnp.bfloat16)
        return carry

    lax.fori_loop(bounds[0], bounds[1], one_tile, 0)
    dk_ref[...] = dk_acc[...].astype(jnp.bfloat16)
    dv_ref[...] = dv_acc[...].astype(jnp.bfloat16)


def attend(q, k, v, g, tags, bounds, halo):
    width = q.shape[0]
    most = 2 * halo + TQ + 2 * TK
    span = -(-min(most, width + TK) // TK) * TK
    vmem = pl.BlockSpec(memory_space=pltpu.VMEM)
    smem = pl.BlockSpec(memory_space=pltpu.SMEM)
    out = jax.ShapeDtypeStruct((width, LANES), jnp.bfloat16)
    return pl.pallas_call(
        attend_kernel,
        out_shape=(out,) * 4,
        in_specs=[smem, smem] + [vmem] * 8,
        out_specs=(vmem,) * 4,
        scratch_shapes=[
            pltpu.VMEM((span, 2 * TQ), jnp.float32),
            pltpu.VMEM((span, 2 * TQ), jnp.float32),
            pltpu.VMEM((width, LANES), jnp.float32),
            pltpu.VMEM((width, LANES), jnp.float32),
            pltpu.VMEM((LANES, 2 * TQ), jnp.float32),
            pltpu.VMEM((LANES, 2 * TQ), jnp.float32),
        ],
        compiler_params=pltpu.CompilerParams(vmem_limit_bytes=56 * 1024 * 1024),
        cost_estimate=pl.CostEstimate(
            flops=60_000_000_000, bytes_accessed=12_000_000, transcendentals=8_000_000),
    )(tags, bounds, q, k, v, g, k.T, v.T,
      jnp.broadcast_to(tags[:, None], (width, LANES)), tags.reshape(width // LANES, LANES))


def shards(queries, keys, values, out_grad, image_ids):
    row_count, features = queries.shape
    count = lax.axis_size("img")
    team = features // LANES
    groups = [list(range(at, at + team)) for at in range(0, count, team)]
    own = team * row_count
    halo = REACH * row_count
    down = [(i, i - team) for i in range(team, count)]
    up = [(i, i + team) for i in range(count - team)]

    def gather(x):
        x = x.reshape(row_count, team, LANES).transpose(1, 0, 2)
        x = lax.all_to_all(x, "img", 0, 0, axis_index_groups=groups)
        x = x.reshape(own, LANES)
        far = lax.ppermute(x[:halo], "img", down)
        return jnp.concatenate([x, far, jnp.zeros((TK - LANES, LANES), x.dtype)], 0)

    tags = lax.all_gather(image_ids, "img", tiled=True) + 1
    start = (lax.axis_index("img") // team) * own
    padded = jnp.concatenate(
        [jnp.zeros((1,), jnp.int32), tags, jnp.full((halo + TK - LANES,), NO_TAG, jnp.int32)])
    width = own + halo + TK - LANES
    before = lax.dynamic_slice_in_dim(padded, start, 1)[0]
    window = lax.dynamic_slice_in_dim(padded, start + 1, width)
    window = jnp.where(jnp.arange(width) < own + halo, window, NO_TAG)
    first = jnp.sum((window == before).astype(jnp.int32))
    last = jnp.sum((window <= window[own - 1]).astype(jnp.int32))
    bounds = jnp.stack([first // TQ, (last + TQ - 1) // TQ]).astype(jnp.int32)

    results = attend(*(gather(x) for x in (queries, keys, values, out_grad)), window, bounds, halo)
    from_below = (window[:halo] == before)[:, None]

    def give_back(x):
        far = lax.ppermute(x[own : own + halo], "img", up)
        x = jnp.concatenate([jnp.where(from_below, far, x[:halo]), x[halo:own]], 0)
        x = lax.all_to_all(
            x.reshape(team, row_count, LANES), "img", 0, 0, axis_index_groups=groups)
        return x.transpose(1, 0, 2).reshape(row_count, features)

    return tuple(give_back(x) for x in results)


def solution(mesh):
    in_specs = (P("img", None), P("img", None), P("img", None), P("img", None), P("img"))
    out_specs = (P("img", None), P("img", None), P("img", None), P("img", None))
    return jax.shard_map(shards, mesh=mesh, in_specs=in_specs, out_specs=out_specs, check_vma=False)
```

```python
import math

import jax
import jax.numpy as jnp
from jax import lax
from jax.experimental import pallas as pl
from jax.experimental.pallas import tpu as pltpu
from jax.sharding import PartitionSpec as P

HEAD_DIM = 64
REACH = 3
LANES = 128
TQ = 128
TK = 256
NO_TAG = 1 << 30


def dot_nt(a, b):
    return lax.dot_general(a, b, (((1,), (1,)), ((), ())), preferred_element_type=jnp.float32)


def dot_nn(a, b):
    return lax.dot_general(a, b, (((1,), (0,)), ((), ())), preferred_element_type=jnp.float32)


def attend_kernel(
    tags_s, bounds, q_ref, k_ref, v_ref, g_ref, kt_ref, vt_ref, tag_cols, tag_rows,
    att_ref, dq_ref, dk_ref, dv_ref,
    s_buf, dp_buf, dk_acc, dv_acc, att_acc, dq_acc,
):
    dk_acc[...] = jnp.zeros_like(dk_acc)
    dv_acc[...] = jnp.zeros_like(dv_acc)
    low = lax.broadcasted_iota(jnp.int32, (TQ, LANES), 1) < HEAD_DIM
    scale = 1.0 / math.sqrt(HEAD_DIM)
    all_tags = tag_rows[...]

    def one_tile(tile, carry):
        row0 = pl.multiple_of(tile * TQ, TQ)
        rows = pl.ds(row0, TQ)
        first_tag = tags_s[row0]
        last_tag = tags_s[row0 + TQ - 1]
        key_begin = jnp.sum((all_tags < first_tag).astype(jnp.int32))
        key_end = jnp.sum((all_tags <= last_tag).astype(jnp.int32))
        key0 = (key_begin // LANES) * LANES
        steps = (key_end - key0 + TK - 1) // TK
        key0 = jnp.minimum(key0, k_ref.shape[0] - steps * TK)
        q = q_ref[rows, :].astype(jnp.float32) * scale
        g = g_ref[rows, :].astype(jnp.float32)
        q2 = jnp.concatenate(
            [jnp.where(low, q, 0.0), jnp.where(low, 0.0, q)], 0).astype(jnp.bfloat16)
        g2 = jnp.concatenate(
            [jnp.where(low, g, 0.0), jnp.where(low, 0.0, g)], 0).astype(jnp.bfloat16)
        q_tags = tag_rows[pl.ds(tile, 1), :]

        def score_step(j, peak):
            keys = pl.ds(pl.multiple_of(key0 + j * TK, LANES), TK)
            held = pl.ds(pl.multiple_of(j * TK, TK), TK)
            s = dot_nt(k_ref[keys, :], q2)
            same = tag_cols[keys, :] == q_tags
            s = jnp.concatenate(
                [jnp.where(same, s[:, :TQ], -1e30), jnp.where(same, s[:, TQ:], -1e30)], 1)
            s_buf[held, :] = s
            dp_buf[held, :] = dot_nt(v_ref[keys, :], g2)
            return jnp.maximum(peak, jnp.max(s.reshape(TK // 8, 8, 2 * TQ), 0))

        peak = lax.fori_loop(0, steps, score_step, jnp.full((8, 2 * TQ), -1e30, jnp.float32))
        peak = jnp.max(peak, 0, keepdims=True)

        def weight_step(j, sums):
            total, delta = sums
            held = pl.ds(pl.multiple_of(j * TK, TK), TK)
            w = jnp.exp(s_buf[held, :] - peak)
            s_buf[held, :] = w
            wd = w * dp_buf[held, :]
            total = total + jnp.sum(w.reshape(TK // 8, 8, 2 * TQ), 0)
            delta = delta + jnp.sum(wd.reshape(TK // 8, 8, 2 * TQ), 0)
            return total, delta

        zero = jnp.zeros((8, 2 * TQ), jnp.float32)
        total, delta = lax.fori_loop(0, steps, weight_step, (zero, zero))
        inverse = 1.0 / jnp.sum(total, 0, keepdims=True)
        delta = jnp.sum(delta, 0, keepdims=True) * inverse
        att_acc[...] = jnp.zeros_like(att_acc)
        dq_acc[...] = jnp.zeros_like(dq_acc)

        def grad_step(j, c):
            keys = pl.ds(pl.multiple_of(key0 + j * TK, LANES), TK)
            held = pl.ds(pl.multiple_of(j * TK, TK), TK)
            p = s_buf[held, :] * inverse
            ds = (p * (dp_buf[held, :] - delta)).astype(jnp.bfloat16)
            p = p.astype(jnp.bfloat16)
            att_acc[...] += dot_nn(vt_ref[:, keys], p)
            dq_acc[...] += dot_nn(kt_ref[:, keys], ds)
            dv_acc[keys, :] += dot_nn(p, g2)
            dk_acc[keys, :] += dot_nn(ds, q2)
            return c

        lax.fori_loop(0, steps, grad_step, 0)
        att = att_acc[...]
        dq = dq_acc[...] * scale
        top = lax.broadcasted_iota(jnp.int32, (LANES, TQ), 0) < HEAD_DIM
        att_ref[rows, :] = jnp.where(top, att[:, :TQ], att[:, TQ:]).T.astype(jnp.bfloat16)
        dq_ref[rows, :] = jnp.where(top, dq[:, :TQ], dq[:, TQ:]).T.astype(jnp.bfloat16)
        return carry

    lax.fori_loop(bounds[0], bounds[1], one_tile, 0)
    dk_ref[...] = dk_acc[...].astype(jnp.bfloat16)
    dv_ref[...] = dv_acc[...].astype(jnp.bfloat16)


def attend(q, k, v, g, tags, bounds, halo):
    width = q.shape[0]
    most = 2 * halo + TQ + 2 * TK
    span = -(-min(most, width + TK) // TK) * TK
    vmem = pl.BlockSpec(memory_space=pltpu.VMEM)
    smem = pl.BlockSpec(memory_space=pltpu.SMEM)
    out = jax.ShapeDtypeStruct((width, LANES), jnp.bfloat16)
    return pl.pallas_call(
        attend_kernel,
        out_shape=(out,) * 4,
        in_specs=[smem, smem] + [vmem] * 8,
        out_specs=(vmem,) * 4,
        scratch_shapes=[
            pltpu.VMEM((span, 2 * TQ), jnp.float32),
            pltpu.VMEM((span, 2 * TQ), jnp.float32),
            pltpu.VMEM((width, LANES), jnp.float32),
            pltpu.VMEM((width, LANES), jnp.float32),
            pltpu.VMEM((LANES, 2 * TQ), jnp.float32),
            pltpu.VMEM((LANES, 2 * TQ), jnp.float32),
        ],
        compiler_params=pltpu.CompilerParams(vmem_limit_bytes=56 * 1024 * 1024),
        cost_estimate=pl.CostEstimate(
            flops=60_000_000_000, bytes_accessed=12_000_000, transcendentals=8_000_000),
    )(tags, bounds, q, k, v, g, k.T, v.T,
      jnp.broadcast_to(tags[:, None], (width, LANES)), tags.reshape(width // LANES, LANES))


MESH = pl.DeviceIdType.MESH


def greet(me, base, pos, team, up, down):
    barrier = pltpu.get_barrier_semaphore()
    for step in range(1, team):
        mate = base + lax.rem(pos + step, team)
        pl.semaphore_signal(barrier, inc=1, device_id=(mate,), device_id_type=MESH)
    pl.semaphore_signal(barrier, inc=1, device_id=(up,), device_id_type=MESH)
    pl.semaphore_signal(barrier, inc=1, device_id=(down,), device_id_type=MESH)
    pl.semaphore_wait(barrier, team + 1)


def place(count, team):
    me = lax.axis_index("img")
    pos = lax.rem(me, team)
    return me, me - pos, pos, lax.rem(me + team, count), lax.rem(me + count - team, count)


def remote(src, dst, send_sem, recv_sem, device):
    copy = pltpu.make_async_remote_copy(
        src_ref=src, dst_ref=dst, send_sem=send_sem, recv_sem=recv_sem,
        device_id=(device,), device_id_type=MESH)
    return copy


def lanes_of(pos):
    return pl.ds(pl.multiple_of(pos * LANES, LANES), LANES)


def gather_kernel(count, team, *refs):
    ins, outs = refs[:5], refs[5:10]
    send, recv, halo_send, halo_recv = refs[10:]
    me, base, pos, up, down = place(count, team)
    greet(me, base, pos, team, up, down)
    copies = []
    for t, (src, dst) in enumerate(zip(ins, outs)):
        rows = src.shape[0]
        mine = pl.ds(pl.multiple_of(pos * rows, 8), rows)
        for step in range(1, team):
            mate = lax.rem(pos + step, team)
            part = src if t == 0 else src.at[:, lanes_of(mate)]
            copy = remote(
                part, dst.at[mine, :], send.at[t, step], recv.at[t, step], base + mate)
            copy.start()
            copies.append(copy)
    for t, (src, dst) in enumerate(zip(ins, outs)):
        rows = src.shape[0]
        mine = pl.ds(pl.multiple_of(pos * rows, 8), rows)
        dst[mine, :] = src[...] if t == 0 else src[:, lanes_of(pos)]
    later = []
    for t, dst in enumerate(outs):
        rows = ins[t].shape[0]
        for copy in copies[t * (team - 1) : (t + 1) * (team - 1)]:
            copy.wait_recv()
        copy = remote(
            dst.at[pl.ds(0, REACH * rows), :], dst.at[pl.ds(team * rows, REACH * rows), :],
            halo_send.at[t], halo_recv.at[t], down)
        copy.start()
        later.append(copy)
        if t == 0:
            copy = remote(
                dst.at[pl.ds((team - 1) * rows, rows), :],
                dst.at[pl.ds((team + REACH) * rows, rows), :],
                halo_send.at[5], halo_recv.at[5], up)
            copy.start()
            later.append(copy)
    for copy in later:
        copy.wait()
    for copy in copies:
        copy.wait_send()


def gather(count, team, tags, arrays):
    rows = arrays[0].shape[0]
    vmem = pl.BlockSpec(memory_space=pltpu.VMEM)
    width = (team + REACH) * rows
    tag_rows = (team + REACH + 1) * tags.shape[0]
    return pl.pallas_call(
        lambda *refs: gather_kernel(count, team, *refs),
        out_shape=(jax.ShapeDtypeStruct((tag_rows, LANES), jnp.int32),)
        + (jax.ShapeDtypeStruct((width, LANES), jnp.bfloat16),) * 4,
        in_specs=[vmem] * 5,
        out_specs=(vmem,) * 5,
        scratch_shapes=[
            pltpu.SemaphoreType.DMA((5, team)),
            pltpu.SemaphoreType.DMA((5, team)),
            pltpu.SemaphoreType.DMA((6,)),
            pltpu.SemaphoreType.DMA((6,)),
        ],
        compiler_params=pltpu.CompilerParams(collective_id=0, has_side_effects=True),
        name="gather",
    )(tags, *arrays)


def scatter_kernel(count, team, *refs):
    below, ins, outs = refs[0], refs[1:5], refs[5:9]
    far, staged, send, recv, halo_send, halo_recv = refs[9:]
    me, base, pos, up, down = place(count, team)
    rows = outs[0].shape[0]
    halo = REACH * rows
    greet(me, base, pos, team, up, down)
    halos = []
    for t, src in enumerate(ins):
        copy = remote(
            src.at[pl.ds(team * rows, halo), :], far.at[t], halo_send.at[t], halo_recv.at[t], up)
        copy.start()
        halos.append(copy)

    def block(t, step, early):
        mate = lax.rem(pos + step, team)
        at = pl.ds(pl.multiple_of(mate * rows, 16), rows) if early else pl.ds(
            pl.multiple_of(lax.rem(mate, REACH) * rows, 16), rows)
        src = ins[t].at[at, :] if early else staged.at[t, at, :]
        return remote(
            src, outs[t].at[:, lanes_of(pos)], send.at[t, step], recv.at[t, step], base + mate)

    for t in range(4):
        for step in range(1, team):
            @pl.when(lax.rem(pos + step, team) >= REACH)
            def _():
                block(t, step, True).start()

    for t in range(4):
        halos[t].wait_recv()

        def choose(i, c):
            at = pl.ds(pl.multiple_of(i * LANES, LANES), LANES)
            mixed = jnp.where(
                below[at, :] > 0, far[t, at, :].astype(jnp.float32),
                ins[t][at, :].astype(jnp.float32))
            staged[t, at, :] = mixed.astype(jnp.bfloat16)
            return c

        lax.fori_loop(0, halo // LANES, choose, 0)
        for step in range(1, team):
            @pl.when(lax.rem(pos + step, team) < REACH)
            def _():
                block(t, step, False).start()

    @pl.when(pos < REACH)
    def _():
        for t in range(4):
            at = pl.ds(pl.multiple_of(lax.rem(pos, REACH) * rows, 16), rows)
            outs[t][:, lanes_of(pos)] = staged[t, at, :]

    @pl.when(pos >= REACH)
    def _():
        for t in range(4):
            outs[t][:, lanes_of(pos)] = ins[t][pl.ds(pl.multiple_of(pos * rows, 16), rows), :]

    for t in range(4):
        for step in range(1, team):
            copy = block(t, step, True)
            copy.wait_recv()
            copy.wait_send()
        halos[t].wait_send()


def scatter(count, team, below, arrays):
    halo = below.shape[0]
    rows = halo // REACH
    vmem = pl.BlockSpec(memory_space=pltpu.VMEM)
    return pl.pallas_call(
        lambda *refs: scatter_kernel(count, team, *refs),
        out_shape=(jax.ShapeDtypeStruct((rows, team * LANES), jnp.bfloat16),) * 4,
        in_specs=[vmem] * 5,
        out_specs=(vmem,) * 4,
        scratch_shapes=[
            pltpu.VMEM((4, halo, LANES), jnp.bfloat16),
            pltpu.VMEM((4, halo, LANES), jnp.bfloat16),
            pltpu.SemaphoreType.DMA((4, team)),
            pltpu.SemaphoreType.DMA((4, team)),
            pltpu.SemaphoreType.DMA((4,)),
            pltpu.SemaphoreType.DMA((4,)),
        ],
        compiler_params=pltpu.CompilerParams(collective_id=1, has_side_effects=True),
        name="scatter",
    )(below, *arrays)


def shards(queries, keys, values, out_grad, image_ids):
    row_count, features = queries.shape
    count = lax.axis_size("img")
    team = features // LANES
    own = team * row_count
    halo = REACH * row_count
    width = own + halo

    tag_block = jnp.pad((image_ids + 1).reshape(row_count // LANES, LANES),
                        ((0, 8 - row_count // LANES), (0, 0)))
    tags, k, v, q, g = gather(count, team, tag_block, (keys, values, queries, out_grad))
    me = lax.axis_index("img")
    tags = tags.reshape(team + REACH + 1, 8, LANES)[:, : row_count // LANES].reshape(-1)
    before = jnp.where(me < team, 0, tags[-1])
    window = jnp.where((me >= count - team) & (jnp.arange(width) >= own), NO_TAG, tags[:width])
    first = jnp.sum((window == before).astype(jnp.int32))
    last = jnp.sum((window <= window[own - 1]).astype(jnp.int32))
    bounds = jnp.stack([first // TQ, (last + TQ - 1) // TQ]).astype(jnp.int32)
    results = attend(q, k, v, g, window, bounds, halo)
    below = jnp.broadcast_to((window[:halo] == before).astype(jnp.int32)[:, None], (halo, LANES))
    return scatter(count, team, below, results)


def solution(mesh):
    in_specs = (P("img", None), P("img", None), P("img", None), P("img", None), P("img"))
    out_specs = (P("img", None), P("img", None), P("img", None), P("img", None))
    return jax.shard_map(shards, mesh=mesh, in_specs=in_specs, out_specs=out_specs, check_vma=False)
```

```python
import math

import jax
import jax.numpy as jnp
from jax import lax
from jax.experimental import pallas as pl
from jax.experimental.pallas import tpu as pltpu
from jax.sharding import PartitionSpec as P

HEAD_DIM = 64
REACH = 3
LANES = 128
TQ = 128
TK = 768
NO_TAG = 1 << 30


def dot_nt(a, b):
    return lax.dot_general(a, b, (((1,), (1,)), ((), ())), preferred_element_type=jnp.float32)


def dot_nn(a, b):
    return lax.dot_general(a, b, (((1,), (0,)), ((), ())), preferred_element_type=jnp.float32)


def attend_kernel(
    begins, ends, bounds, q_ref, k_ref, v_ref, g_ref, kt_ref, vt_ref, tag_cols, tag_rows,
    att_ref, dq_ref, dk_ref, dv_ref,
    s_buf, dp_buf, dk_acc, dv_acc, att_acc, dq_acc,
):
    dk_acc[...] = jnp.zeros_like(dk_acc)
    dv_acc[...] = jnp.zeros_like(dv_acc)
    low = lax.broadcasted_iota(jnp.int32, (TQ, LANES), 1) < HEAD_DIM
    scale = 1.0 / math.sqrt(HEAD_DIM)

    def one_tile(tile, carry):
        row0 = pl.multiple_of(tile * TQ, TQ)
        rows = pl.ds(row0, TQ)
        key_begin = begins[tile]
        key_end = ends[tile]
        key0 = (key_begin // LANES) * LANES
        steps = (key_end - key0 + TK - 1) // TK
        key0 = jnp.minimum(key0, k_ref.shape[0] - steps * TK)
        q = q_ref[rows, :].astype(jnp.float32) * scale
        g = g_ref[rows, :].astype(jnp.float32)
        q2 = jnp.concatenate(
            [jnp.where(low, q, 0.0), jnp.where(low, 0.0, q)], 0).astype(jnp.bfloat16)
        g2 = jnp.concatenate(
            [jnp.where(low, g, 0.0), jnp.where(low, 0.0, g)], 0).astype(jnp.bfloat16)
        q_tags = tag_rows[pl.ds(tile, 1), :]

        def score_step(j, peak):
            keys = pl.ds(pl.multiple_of(key0 + j * TK, LANES), TK)
            held = pl.ds(pl.multiple_of(j * TK, TK), TK)
            s = dot_nt(k_ref[keys, :], q2)
            same = tag_cols[keys, :] == q_tags
            s = jnp.concatenate(
                [jnp.where(same, s[:, :TQ], -1e30), jnp.where(same, s[:, TQ:], -1e30)], 1)
            s_buf[held, :] = s
            dp_buf[held, :] = dot_nt(v_ref[keys, :], g2)
            return jnp.maximum(peak, jnp.max(s.reshape(TK // 8, 8, 2 * TQ), 0))

        peak = lax.fori_loop(0, steps, score_step, jnp.full((8, 2 * TQ), -1e30, jnp.float32))
        peak = jnp.max(peak, 0, keepdims=True)

        def weight_step(j, sums):
            total, delta = sums
            held = pl.ds(pl.multiple_of(j * TK, TK), TK)
            w = jnp.exp(s_buf[held, :] - peak)
            s_buf[held, :] = w
            wd = w * dp_buf[held, :]
            total = total + jnp.sum(w.reshape(TK // 8, 8, 2 * TQ), 0)
            delta = delta + jnp.sum(wd.reshape(TK // 8, 8, 2 * TQ), 0)
            return total, delta

        zero = jnp.zeros((8, 2 * TQ), jnp.float32)
        total, delta = lax.fori_loop(0, steps, weight_step, (zero, zero))
        inverse = 1.0 / jnp.sum(total, 0, keepdims=True)
        delta = jnp.sum(delta, 0, keepdims=True) * inverse
        att_acc[...] = jnp.zeros_like(att_acc)
        dq_acc[...] = jnp.zeros_like(dq_acc)

        def grad_step(j, c):
            keys = pl.ds(pl.multiple_of(key0 + j * TK, LANES), TK)
            held = pl.ds(pl.multiple_of(j * TK, TK), TK)
            p = s_buf[held, :] * inverse
            ds = (p * (dp_buf[held, :] - delta)).astype(jnp.bfloat16)
            p = p.astype(jnp.bfloat16)
            att_acc[...] += dot_nn(vt_ref[:, keys], p)
            dq_acc[...] += dot_nn(kt_ref[:, keys], ds)
            dv_acc[keys, :] += dot_nn(p, g2)
            dk_acc[keys, :] += dot_nn(ds, q2)
            return c

        lax.fori_loop(0, steps, grad_step, 0)
        att = att_acc[...]
        dq = dq_acc[...] * scale
        top = lax.broadcasted_iota(jnp.int32, (LANES, TQ), 0) < HEAD_DIM
        att_ref[rows, :] = jnp.where(top, att[:, :TQ], att[:, TQ:]).T.astype(jnp.bfloat16)
        dq_ref[rows, :] = jnp.where(top, dq[:, :TQ], dq[:, TQ:]).T.astype(jnp.bfloat16)
        return carry

    lax.fori_loop(bounds[0], bounds[1], one_tile, 0)
    dk_ref[...] = dk_acc[...].astype(jnp.bfloat16)
    dv_ref[...] = dv_acc[...].astype(jnp.bfloat16)


def attend(q, k, v, g, tags, bounds, halo):
    width = q.shape[0]
    most = 2 * halo + TQ + 2 * TK
    span = -(-min(most, width + TK) // TK) * TK
    vmem = pl.BlockSpec(memory_space=pltpu.VMEM)
    smem = pl.BlockSpec(memory_space=pltpu.SMEM)
    begins = jnp.sum((tags[None, :] < tags[::TQ][:, None]).astype(jnp.int32), 1)
    ends = jnp.sum((tags[None, :] <= tags[TQ - 1 :: TQ][:, None]).astype(jnp.int32), 1)
    out = jax.ShapeDtypeStruct((width, LANES), jnp.bfloat16)
    return pl.pallas_call(
        attend_kernel,
        out_shape=(out,) * 4,
        in_specs=[smem] * 3 + [vmem] * 8,
        out_specs=(vmem,) * 4,
        scratch_shapes=[
            pltpu.VMEM((span, 2 * TQ), jnp.float32),
            pltpu.VMEM((span, 2 * TQ), jnp.float32),
            pltpu.VMEM((width, LANES), jnp.float32),
            pltpu.VMEM((width, LANES), jnp.float32),
            pltpu.VMEM((LANES, 2 * TQ), jnp.float32),
            pltpu.VMEM((LANES, 2 * TQ), jnp.float32),
        ],
        compiler_params=pltpu.CompilerParams(vmem_limit_bytes=56 * 1024 * 1024),
        cost_estimate=pl.CostEstimate(
            flops=60_000_000_000, bytes_accessed=12_000_000, transcendentals=8_000_000),
    )(begins, ends, bounds, q, k, v, g, k.T, v.T,
      jnp.broadcast_to(tags[:, None], (width, LANES)), tags.reshape(width // LANES, LANES))


MESH = pl.DeviceIdType.MESH


def greet(me, base, pos, team, up, down):
    barrier = pltpu.get_barrier_semaphore()
    for step in range(1, team):
        mate = base + lax.rem(pos + step, team)
        pl.semaphore_signal(barrier, inc=1, device_id=(mate,), device_id_type=MESH)
    pl.semaphore_signal(barrier, inc=1, device_id=(up,), device_id_type=MESH)
    pl.semaphore_signal(barrier, inc=1, device_id=(down,), device_id_type=MESH)
    pl.semaphore_wait(barrier, team + 1)


def place(count, team):
    me = lax.axis_index("img")
    pos = lax.rem(me, team)
    return me, me - pos, pos, lax.rem(me + team, count), lax.rem(me + count - team, count)


def remote(src, dst, send_sem, recv_sem, device):
    copy = pltpu.make_async_remote_copy(
        src_ref=src, dst_ref=dst, send_sem=send_sem, recv_sem=recv_sem,
        device_id=(device,), device_id_type=MESH)
    return copy


def lanes_of(pos):
    return pl.ds(pl.multiple_of(pos * LANES, LANES), LANES)


def gather_kernel(count, team, *refs):
    ins, outs = refs[:5], refs[5:10]
    send, recv, halo_send, halo_recv = refs[10:]
    me, base, pos, up, down = place(count, team)
    greet(me, base, pos, team, up, down)
    copies = []
    for t, (src, dst) in enumerate(zip(ins, outs)):
        rows = src.shape[0]
        mine = pl.ds(pl.multiple_of(pos * rows, 8), rows)
        for step in range(1, team):
            mate = lax.rem(pos + step, team)
            part = src if t == 0 else src.at[:, lanes_of(mate)]
            copy = remote(
                part, dst.at[mine, :], send.at[t, step], recv.at[t, step], base + mate)
            copy.start()
            copies.append(copy)
    for t, (src, dst) in enumerate(zip(ins, outs)):
        rows = src.shape[0]
        mine = pl.ds(pl.multiple_of(pos * rows, 8), rows)
        dst[mine, :] = src[...] if t == 0 else src[:, lanes_of(pos)]
    later = []
    for t, dst in enumerate(outs):
        rows = ins[t].shape[0]
        for copy in copies[t * (team - 1) : (t + 1) * (team - 1)]:
            copy.wait_recv()
        copy = remote(
            dst.at[pl.ds(0, REACH * rows), :], dst.at[pl.ds(team * rows, REACH * rows), :],
            halo_send.at[t], halo_recv.at[t], down)
        copy.start()
        later.append(copy)
        if t == 0:
            copy = remote(
                dst.at[pl.ds((team - 1) * rows, rows), :],
                dst.at[pl.ds((team + REACH) * rows, rows), :],
                halo_send.at[5], halo_recv.at[5], up)
            copy.start()
            later.append(copy)
    for copy in later:
        copy.wait()
    for copy in copies:
        copy.wait_send()


def gather(count, team, tags, arrays):
    rows = arrays[0].shape[0]
    vmem = pl.BlockSpec(memory_space=pltpu.VMEM)
    width = (team + REACH) * rows
    tag_rows = (team + REACH + 1) * tags.shape[0]
    return pl.pallas_call(
        lambda *refs: gather_kernel(count, team, *refs),
        out_shape=(jax.ShapeDtypeStruct((tag_rows, LANES), jnp.int32),)
        + (jax.ShapeDtypeStruct((width, LANES), jnp.bfloat16),) * 4,
        in_specs=[vmem] * 5,
        out_specs=(vmem,) * 5,
        scratch_shapes=[
            pltpu.SemaphoreType.DMA((5, team)),
            pltpu.SemaphoreType.DMA((5, team)),
            pltpu.SemaphoreType.DMA((6,)),
            pltpu.SemaphoreType.DMA((6,)),
        ],
        compiler_params=pltpu.CompilerParams(collective_id=0, has_side_effects=True),
        name="gather",
    )(tags, *arrays)


def scatter_kernel(count, team, *refs):
    below, ins, outs = refs[0], refs[1:5], refs[5:9]
    far, staged, send, recv, halo_send, halo_recv = refs[9:]
    me, base, pos, up, down = place(count, team)
    rows = outs[0].shape[0]
    halo = REACH * rows
    greet(me, base, pos, team, up, down)
    halos = []
    for t, src in enumerate(ins):
        copy = remote(
            src.at[pl.ds(team * rows, halo), :], far.at[t], halo_send.at[t], halo_recv.at[t], up)
        copy.start()
        halos.append(copy)

    def block(t, step, early):
        mate = lax.rem(pos + step, team)
        at = pl.ds(pl.multiple_of(mate * rows, 16), rows) if early else pl.ds(
            pl.multiple_of(lax.rem(mate, REACH) * rows, 16), rows)
        src = ins[t].at[at, :] if early else staged.at[t, at, :]
        return remote(
            src, outs[t].at[:, lanes_of(pos)], send.at[t, step], recv.at[t, step], base + mate)

    for t in range(4):
        for step in range(1, team):
            @pl.when(lax.rem(pos + step, team) >= REACH)
            def _():
                block(t, step, True).start()

    for t in range(4):
        halos[t].wait_recv()

        def choose(i, c):
            at = pl.ds(pl.multiple_of(i * LANES, LANES), LANES)
            mixed = jnp.where(
                below[at, :] > 0, far[t, at, :].astype(jnp.float32),
                ins[t][at, :].astype(jnp.float32))
            staged[t, at, :] = mixed.astype(jnp.bfloat16)
            return c

        lax.fori_loop(0, halo // LANES, choose, 0)
        for step in range(1, team):
            @pl.when(lax.rem(pos + step, team) < REACH)
            def _():
                block(t, step, False).start()

    @pl.when(pos < REACH)
    def _():
        for t in range(4):
            at = pl.ds(pl.multiple_of(lax.rem(pos, REACH) * rows, 16), rows)
            outs[t][:, lanes_of(pos)] = staged[t, at, :]

    @pl.when(pos >= REACH)
    def _():
        for t in range(4):
            outs[t][:, lanes_of(pos)] = ins[t][pl.ds(pl.multiple_of(pos * rows, 16), rows), :]

    for t in range(4):
        for step in range(1, team):
            copy = block(t, step, True)
            copy.wait_recv()
            copy.wait_send()
        halos[t].wait_send()


def scatter(count, team, below, arrays):
    halo = below.shape[0]
    rows = halo // REACH
    vmem = pl.BlockSpec(memory_space=pltpu.VMEM)
    return pl.pallas_call(
        lambda *refs: scatter_kernel(count, team, *refs),
        out_shape=(jax.ShapeDtypeStruct((rows, team * LANES), jnp.bfloat16),) * 4,
        in_specs=[vmem] * 5,
        out_specs=(vmem,) * 4,
        scratch_shapes=[
            pltpu.VMEM((4, halo, LANES), jnp.bfloat16),
            pltpu.VMEM((4, halo, LANES), jnp.bfloat16),
            pltpu.SemaphoreType.DMA((4, team)),
            pltpu.SemaphoreType.DMA((4, team)),
            pltpu.SemaphoreType.DMA((4,)),
            pltpu.SemaphoreType.DMA((4,)),
        ],
        compiler_params=pltpu.CompilerParams(collective_id=1, has_side_effects=True),
        name="scatter",
    )(below, *arrays)


def shards(queries, keys, values, out_grad, image_ids):
    row_count, features = queries.shape
    count = lax.axis_size("img")
    team = features // LANES
    own = team * row_count
    halo = REACH * row_count
    width = own + halo

    tag_block = jnp.pad((image_ids + 1).reshape(row_count // LANES, LANES),
                        ((0, 8 - row_count // LANES), (0, 0)))
    tags, k, v, q, g = gather(count, team, tag_block, (keys, values, queries, out_grad))
    me = lax.axis_index("img")
    tags = tags.reshape(team + REACH + 1, 8, LANES)[:, : row_count // LANES].reshape(-1)
    before = jnp.where(me < team, 0, tags[-1])
    window = jnp.where((me >= count - team) & (jnp.arange(width) >= own), NO_TAG, tags[:width])
    first = jnp.sum((window == before).astype(jnp.int32))
    last = jnp.sum((window <= window[own - 1]).astype(jnp.int32))
    bounds = jnp.stack([first // TQ, (last + TQ - 1) // TQ]).astype(jnp.int32)
    results = attend(q, k, v, g, window, bounds, halo)
    below = jnp.broadcast_to((window[:halo] == before).astype(jnp.int32)[:, None], (halo, LANES))
    return scatter(count, team, below, results)


def solution(mesh):
    in_specs = (P("img", None), P("img", None), P("img", None), P("img", None), P("img"))
    out_specs = (P("img", None), P("img", None), P("img", None), P("img", None))
    return jax.shard_map(shards, mesh=mesh, in_specs=in_specs, out_specs=out_specs, check_vma=False)
```
